128 devices in a mesh: rows: 128 (over y, z, x, core).
Axes of the slice: x: 4, y: 4, z: 4, core: 2. Of those that a mesh axis runs over, the one named last changes fastest.
Arguments:
- right_sides: float32 [32, 131072], P(None, 'rows'), may hold values from -48 to 48
- initial: float32 [32, 131072], P(None, 'rows'), may hold values from -1.2 to 1.2
- diag_blocks: float32 [131072, 256], P('rows'), may hold values from -2 to 9
- sub_blocks: float32 [131072, 256], P('rows'), may hold values from -0.21875 to 0.21875
- super_blocks: float32 [131072, 256], P('rows'), may hold values from -0.21875 to 0.21875
- local_inverse: bfloat16 [131072, 1024], P('rows'), may hold values from -1 to 1
- upper_spikes: bfloat16 [256, 131072], P(None, 'rows'), may hold values from -0.21875 to 0.21875
- lower_spikes: bfloat16 [256, 131072], P(None, 'rows'), may hold values from -2 to 2
Outputs:
- solution: float32 [32, 131072], P(None, 'rows')
- residual_norms: float32 [3, 32], replicated
The draws below stay inside these ranges and needn't reach their ends.
All inputs are finite; a program needn't handle non-finite values.
Results may differ from the reference program's by a relative error of at most 0.002.
The reference program's roundings to bfloat16 on the way (of `rounded`) count: a program that leaves them out, or rounds other values in their place, can miss the bound.
Values may be sent and summed in bfloat16 or wider, within the bound.
A program may use at most 64 MiB of HBM per device.

```python
import math
import jax
import jax.numpy as jnp
from jax import lax

BAND = 256
RHS = 32
ROWS_DEV = 1024
ITERS = 2
ORDER = 131072
N_ROWS = 128


def block_parts(key):
    base_key = jax.random.fold_in(key, 101)
    block_total = ORDER // BAND
    log_scales = jax.random.uniform(jax.random.fold_in(base_key, 1), (block_total, BAND), jnp.float32, math.log(2.0), math.log(8.0))
    mixing = jnp.clip(jax.random.normal(jax.random.fold_in(base_key, 2), (block_total, BAND, BAND), jnp.float32), -5.0, 5.0)
    return (jnp.exp(log_scales), mixing * (0.3 / math.sqrt(BAND)))


def draw_diag_blocks(key, part):
    scales, mixing = block_parts(key)
    unit_matrix = jnp.eye(BAND, dtype=jnp.float32)
    blocks = mixing + scales[:, :, None] * unit_matrix[None]
    return blocks.reshape(ORDER, BAND)


def draw_local_inverse(key, part):
    scales, mixing = block_parts(key)
    inverse_scale = 1.0 / scales
    unit_matrix = jnp.eye(BAND, dtype=jnp.float32)
    approx = inverse_scale[:, :, None] * unit_matrix[None] - inverse_scale[:, :, None] * mixing * inverse_scale[:, None, :]
    per_device = ROWS_DEV // BAND
    approx = approx.reshape(N_ROWS, per_device, BAND, BAND)
    positioned_rows = jnp.einsum('pkij,kl->pkilj', approx, jnp.eye(per_device, dtype=jnp.float32))
    noise = jnp.clip(jax.random.normal(jax.random.fold_in(key, 102), (N_ROWS, ROWS_DEV, ROWS_DEV), jnp.float32), -5.0, 5.0)
    whole = positioned_rows.reshape(N_ROWS, ROWS_DEV, ROWS_DEV) + noise * (0.06 / math.sqrt(ROWS_DEV))
    return jnp.clip(whole.reshape(ORDER, ROWS_DEV), -1.0, 1.0).astype(jnp.bfloat16)


def draw_lower_spikes(key, part):
    inner = jnp.clip(jax.random.normal(jax.random.fold_in(key, 21), (BAND, N_ROWS, ROWS_DEV - BAND), jnp.float32), -5.0, 5.0)
    inner = inner * (0.3 / math.sqrt(BAND))
    slow_share = 0.5
    slowness = jax.random.uniform(jax.random.fold_in(key, 22), (BAND,), jnp.float32) < slow_share
    fast_rate = jnp.exp(jax.random.uniform(jax.random.fold_in(key, 23), (BAND,), jnp.float32, math.log(0.15), math.log(1.0)))
    rates = jnp.where(slowness, 2.5 / N_ROWS, fast_rate)
    spread = jax.random.uniform(jax.random.fold_in(key, 24), (N_ROWS, BAND), jnp.float32, 0.6, 1.4)
    retain = jnp.exp(-rates[None, :] * spread)
    spike_position = jax.random.randint(jax.random.fold_in(key, 25), (3,), 0, N_ROWS)
    eliminated_rows = jnp.any(jnp.arange(N_ROWS)[:, None] == spike_position[None, :], axis=1)
    retain = jnp.where(eliminated_rows[:, None] & slowness[None, :], retain * 0.6, retain)
    mixing = jnp.clip(jax.random.normal(jax.random.fold_in(key, 26), (N_ROWS, BAND, BAND), jnp.float32), -5.0, 5.0)
    coupling = jnp.eye(BAND, dtype=jnp.float32)[None] + mixing * (0.2 / math.sqrt(BAND))
    tip_blocks = -(coupling * retain[:, None, :])
    tip_layout = jnp.transpose(tip_blocks, (1, 0, 2))
    whole = jnp.concatenate([inner, tip_layout], axis=2)
    return jnp.clip(whole.reshape(BAND, ORDER), -2.0, 2.0).astype(jnp.bfloat16)


def draw_right_sides(key, part):
    column = jnp.arange(ORDER, dtype=jnp.float32) / ORDER
    jitter = jax.random.uniform(jax.random.fold_in(key, 31), (ORDER,), jnp.float32, -1.15, 1.15)
    rough = jnp.clip(jax.random.normal(jax.random.fold_in(key, 34), (RHS, ORDER), jnp.float32), -4.0, 4.0)
    column_scale = jnp.exp(math.log(3.0) * column + jitter)
    values = rough * column_scale[None, :]
    return jnp.clip(values, -48.0, 48.0)


def block_levels(stream_key, dims, split, smallest, largest):
    gain = 1.0
    for axis_at, shards_of in split:
        steps = jax.random.uniform(jax.random.fold_in(jax.random.fold_in(stream_key, 6), axis_at), (shards_of,), jnp.float32, smallest / len(split), largest / len(split))
        gain = gain * jnp.repeat(jnp.exp(steps), dims[axis_at] // shards_of).reshape((-1,) + (1,) * (len(dims) - 1 - axis_at))
    return gain


def gaussian(stream_key, extent, width, reach, cuts=(), held_as=jnp.bfloat16):
    loudness = block_levels(stream_key, extent, cuts, -0.22, 0.18) if cuts else 1.0
    entries = jax.random.normal(stream_key, extent, jnp.float32) * width * loudness
    return jnp.minimum(jnp.maximum(entries, -reach), reach).astype(held_as)


def setup_inputs(seed: int = 0) -> dict:
    splits = jax.random.split(jax.random.key(seed), 9)
    return {
        "right_sides": draw_right_sides(jax.random.fold_in(splits[8], 71), 0),
        "initial": gaussian(splits[1], (RHS, ORDER), 0.2, 1.2, ((1, 128),), jnp.float32),
        "diag_blocks": draw_diag_blocks(jax.random.fold_in(splits[8], 71), 0),
        "sub_blocks": gaussian(splits[3], (ORDER, BAND), (3 * BAND) ** -0.5, 0.21875, ((0, 128),), jnp.float32),
        "super_blocks": gaussian(splits[4], (ORDER, BAND), (3 * BAND) ** -0.5, 0.21875, ((0, 128),), jnp.float32),
        "local_inverse": draw_local_inverse(jax.random.fold_in(splits[8], 71), 0),
        "upper_spikes": gaussian(splits[6], (BAND, ORDER), (3 * BAND) ** -0.5, 0.21875, ((1, 128),)),
        "lower_spikes": draw_lower_spikes(jax.random.fold_in(splits[8], 71), 0),
    }


maximum_level = lax.Precision.HIGHEST

def residual_of(right_sides, solution, diag_mat, lower_mat, upper_mat):
    padded = jnp.pad(solution, ((0, 0), (BAND, BAND)))
    stacked = padded.reshape(padded.shape[0], -1, BAND)
    applied = jnp.einsum('rkb,kbc->rkc', stacked[:, 1:-1], diag_mat, precision=maximum_level)
    applied = applied + jnp.einsum('rkb,kbc->rkc', stacked[:, :-2], lower_mat, precision=maximum_level)
    applied = applied + jnp.einsum('rkb,kbc->rkc', stacked[:, 2:], upper_mat, precision=maximum_level)
    return right_sides - applied.reshape(right_sides.shape)

def norm_row(residual):
    return jnp.sqrt(lax.optimization_barrier(jnp.sum(residual * residual, axis=1)) / ORDER)

def solve_partition(operands):
    return jnp.dot(operands[0].astype(jnp.float32), operands[1].astype(jnp.float32), precision=maximum_level)

def advance(carried, operands):
    current = operands[0] + jnp.dot(carried, operands[1], precision=maximum_level)
    return (current, (carried, current))

def rounded_copy(values):
    return lax.optimization_barrier(values.astype(jnp.bfloat16)).astype(jnp.float32)

def reference(right_sides, initial, diag_blocks, sub_blocks, super_blocks, local_inverse, upper_spikes, lower_spikes):
    diag_mat = diag_blocks.reshape(-1, BAND, BAND)
    lower_mat = sub_blocks.reshape(-1, BAND, BAND)
    upper_mat = super_blocks.reshape(-1, BAND, BAND)
    inverse_parts = local_inverse.reshape(N_ROWS, ROWS_DEV, ROWS_DEV)
    upper_pieces = upper_spikes.reshape(BAND, N_ROWS, ROWS_DEV).astype(jnp.float32)
    lower_pieces = lower_spikes.reshape(BAND, N_ROWS, ROWS_DEV).astype(jnp.float32)
    chain_mats = -jnp.transpose(lower_pieces[:, :, ROWS_DEV - BAND:], (1, 0, 2))
    bottom_upper = jnp.transpose(upper_pieces[:, :, ROWS_DEV - BAND:], (1, 0, 2))
    top_lower = jnp.transpose(lower_pieces[:, :, :BAND], (1, 0, 2))
    next_lower = jnp.concatenate([top_lower[1:], jnp.zeros_like(top_lower[:1])], axis=0)
    solution = initial
    records = []
    for turn_index in range(ITERS):
        residual = residual_of(right_sides, solution, diag_mat, lower_mat, upper_mat)
        records.append(norm_row(residual))
        rounded = residual.astype(jnp.bfloat16).reshape(RHS, N_ROWS, ROWS_DEV).transpose(1, 0, 2)
        local_part = lax.map(solve_partition, (rounded, inverse_parts))
        own_top = local_part[:, :, :BAND]
        next_top = jnp.concatenate([own_top[1:], jnp.zeros_like(own_top[:1])], axis=0)
        offset = local_part[:, :, ROWS_DEV - BAND:] - jnp.einsum('pri,pij->prj', next_top, bottom_upper, precision=maximum_level)
        leftover, outputs = lax.scan(advance, jnp.zeros((RHS, BAND), jnp.float32), (offset, chain_mats))
        previous, current = outputs
        top_tip = next_top - jnp.einsum('pri,pij->prj', current, next_lower, precision=maximum_level)
        correction = local_part - jnp.einsum('pri,ipm->prm', rounded_copy(top_tip), upper_pieces, precision=maximum_level)
        correction = correction - jnp.einsum('pri,ipm->prm', rounded_copy(previous), lower_pieces, precision=maximum_level)
        solution = solution + correction.transpose(1, 0, 2).reshape(RHS, ORDER)
    residual = residual_of(right_sides, solution, diag_mat, lower_mat, upper_mat)
    records.append(norm_row(residual))
    return (solution, jnp.stack(records))
```

```python
import functools

import jax
import jax.numpy as jnp
from jax import lax
from jax.experimental import pallas as pl
from jax.experimental.pallas import tpu as pltpu
from jax.sharding import PartitionSpec as P

ITERS = 2
BAND = 256
RHS = 32
COLS = 1024
PARTS = 128
ORDER = 131072
COPIES = 64
MESH = pl.DeviceIdType.MESH
F32 = jnp.float32
BF16 = jnp.bfloat16


def rounded(value):
    return value.astype(BF16)


def two_terms(value):
    high = rounded(value)
    return high, rounded(value - high.astype(F32))


def three_terms(value):
    high = rounded(value)
    rest = value - high.astype(F32)
    middle = rounded(rest)
    return high, middle, rounded(rest - middle.astype(F32))


def dot(a, b):
    return jnp.dot(a, b, preferred_element_type=F32)


def times_exact(value, weight):
    rows = value.shape[0]
    out = dot(jnp.concatenate(three_terms(value), axis=0), weight)
    return out[:rows] + (out[rows : 2 * rows] + out[2 * rows :])


def times_pair(value, high, low):
    rows = value.shape[0]
    terms = jnp.concatenate(three_terms(value), axis=0)
    out = dot(terms, high)
    small = dot(terms[: 2 * rows], low)
    rest = (out[rows : 2 * rows] + out[2 * rows :]) + (small[:rows] + small[rows:])
    return out[:rows] + rest


def matrix_times(a, b):
    a_high, a_low = a
    b_high, b_low = b
    size = a_high.shape[0]
    out = dot(jnp.concatenate([a_high, a_low], axis=0), b_high)
    return out[:size] + (out[size:] + dot(a_high, b_low))


def store_halves(ref, slot, matrix):
    high, low = two_terms(matrix)
    half = BAND // 2
    for k in range(2):
        rows = slice(k * half, (k + 1) * half)
        ref[slot, k, :half, :] = high[rows]
        ref[slot, k, half:, :] = low[rows]


def load_halves(ref, slot):
    half = BAND // 2
    high = jnp.concatenate([ref[slot, 0, :half, :], ref[slot, 1, :half, :]], axis=0)
    low = jnp.concatenate([ref[slot, 0, half:, :], ref[slot, 1, half:, :]], axis=0)
    return high, low


def kernel(
    rhs_hbm, x0_hbm, diag_hbm, sub_hbm, sup_hbm, inv_hbm, up_hbm, low_hbm,
    x_out, norm_out,
    rhs, diag, sub, sup, inv, up, low, a_high, a_low,
    xp, pair_mat, up_before, low_after, gx, gz, gy, mpx, mpz,
    local, next_top, vc, vx, vz, vy, prefix, squares, totals,
    load_sem, send_sem, recv_sem,
):
    me = lax.axis_index("rows")
    core = lax.rem(me, 2)
    ix = lax.rem(me // 2, 4)
    iz = lax.rem(me // 8, 4)
    iy = me // 32
    partner = me + 1 - 2 * core

    def on_x(d):
        return me - 2 * ix + 2 * lax.rem(ix + d, 4)

    def on_z(d):
        return me - 8 * iz + 8 * lax.rem(iz + d, 4)

    def on_y(d):
        return me - 32 * iy + 32 * lax.rem(iy + d, 4)

    has_before = me > 0
    has_after = me < PARTS - 1

    barrier = pltpu.get_barrier_semaphore()
    peers = [partner]
    for d in (1, 2, 3):
        peers += [on_x(d), on_z(d), on_y(d)]
    peers += [lax.rem(me + 1, PARTS), lax.rem(me + PARTS - 1, PARTS)]
    for peer in peers:
        pl.semaphore_signal(barrier, inc=1, device_id=(peer,), device_id_type=MESH)

    loads = {}

    def load(name, source, target):
        copy = pltpu.make_async_copy(source, target, load_sem.at[len(loads)])
        copy.start()
        loads[name] = copy

    last = slice(COLS - BAND, COLS)
    load("pair", low_hbm.at[:, last], pair_mat.at[core])
    load("x0", x0_hbm, xp.at[0, :, BAND : BAND + COLS])
    load("up", up_hbm, up)
    load("low", low_hbm, low)
    load("diag", diag_hbm, diag)
    load("sub", sub_hbm, sub)
    load("sup", sup_hbm, sup)
    load("rhs", rhs_hbm, rhs)
    load("inv", inv_hbm, inv)

    @pl.when(jnp.logical_not(has_before))
    def _():
        up_before[...] = jnp.zeros_like(up_before)
        for k in range(ITERS + 1):
            xp[k, :, :BAND] = jnp.zeros((RHS, BAND), F32)

    @pl.when(jnp.logical_not(has_after))
    def _():
        low_after[...] = jnp.zeros_like(low_after)
        for k in range(ITERS + 1):
            xp[k, :, BAND + COLS :] = jnp.zeros((RHS, BAND), F32)
        for k in range(ITERS):
            next_top[k] = jnp.zeros((RHS, BAND), F32)

    pl.semaphore_wait(barrier, len(peers))

    counter = iter(range(COPIES))
    sent = []

    class Copy:
        def __init__(self, source, target, device, sends=None, receives=None):
            i = next(counter)
            self.copy = pltpu.make_async_remote_copy(
                src_ref=source,
                dst_ref=target,
                send_sem=send_sem.at[i],
                recv_sem=recv_sem.at[i],
                device_id=(device,),
                device_id_type=MESH,
            )
            self.sends, self.receives = sends, receives
            sent.append(self)
            self.guard(sends, self.copy.start)

        def guard(self, condition, action):
            if condition is None:
                action()
            else:
                pl.when(condition)(lambda: action())

        def arrived(self):
            self.guard(self.receives, self.copy.wait_recv)

        def left(self):
            self.guard(self.sends, self.copy.wait_send)

    def to_after(source, target):
        return Copy(source, target, lax.rem(me + 1, PARTS), has_after, has_before)

    def to_before(source, target):
        return Copy(source, target, lax.rem(me + PARTS - 1, PARTS), has_before, has_after)

    def send_edges(k):
        return (
            to_after(xp.at[k, :, COLS : COLS + BAND], xp.at[k, :, :BAND]),
            to_before(xp.at[k, :, BAND : 2 * BAND], xp.at[k, :, BAND + COLS :]),
        )

    loads["pair"].wait()
    pair_copy = Copy(pair_mat.at[core], pair_mat.at[core], partner)
    loads["x0"].wait()
    edges = send_edges(0)
    loads["up"].wait()
    up_copy = to_after(up.at[:, last], up_before)
    loads["low"].wait()
    low_copy = to_before(low.at[:, :BAND], low_after)

    pair_copy.arrived()
    store_halves(gx, ix, dot(pair_mat[0], pair_mat[1]))

    def send_matrix(ref, slot, peer_of, senders=None):
        copies = []
        for d in (1, 2, 3):
            sends, receives = (None, None) if senders is None else senders[d]
            if sends is False:
                continue
            copies.append(
                (d, Copy(ref.at[slot, core], ref.at[slot, core], peer_of(d), sends, receives))
            )
        return copies

    def pass_on(ref, slot, copies):
        passed = []
        for d, copy in copies:
            copy.arrived()
            origin = lax.rem(slot + 4 - d, 4)
            passed.append(
                Copy(ref.at[origin, core], ref.at[origin, core], partner, copy.receives, copy.receives)
            )
        for copy in passed:
            copy.arrived()

    def products(ref, out):
        m = [load_halves(ref, q) for q in range(4)]
        two = two_terms(matrix_times(m[0], m[1]))
        other = two_terms(matrix_times(m[2], m[3]))
        total = matrix_times(two, other)
        return m, two, total

    def store_prefixes(out, m, two):
        row = lax.broadcasted_iota(jnp.int32, (BAND, BAND), 0)
        col = lax.broadcasted_iota(jnp.int32, (BAND, BAND), 1)
        unit = (row == col).astype(F32).astype(BF16)
        three = two_terms(matrix_times(two, m[2]))
        for q, (high, low_term) in enumerate(
            [(unit, jnp.zeros_like(unit)), m[0], two, three]
        ):
            out[q, :BAND, :] = high
            out[q, BAND:, :] = low_term

    x_matrices = send_matrix(gx, ix, on_x)

    for name, source, place in (("sub", sub, 0), ("diag", diag, 1), ("sup", sup, 2)):
        loads[name].wait()
        for m in range(4):
            high, low_term = two_terms(source[m * BAND : (m + 1) * BAND, :])
            rows = slice(place * BAND, (place + 1) * BAND)
            a_high[m, rows, :] = high
            a_low[m, rows, :] = low_term
    loads["rhs"].wait()

    def applied(k, m, first, count):
        start = (m + first) * BAND
        value = xp[k, :, start : start + count * BAND]
        rows = slice(first * BAND, (first + count) * BAND)
        return times_pair(value, a_high[m, rows, :], a_low[m, rows, :])

    def residual(k, halos):
        parts = [
            applied(k, 0, 1, 2),
            applied(k, 1, 0, 3),
            applied(k, 2, 0, 3),
            applied(k, 3, 0, 2),
        ]
        for copy in halos:
            copy.arrived()
        parts[0] = parts[0] + applied(k, 0, 0, 1)
        parts[3] = parts[3] + applied(k, 3, 2, 1)
        parts = [rhs[:, m * BAND : (m + 1) * BAND] - parts[m] for m in range(4)]
        total = jnp.zeros((RHS, 128), F32)
        for part in parts:
            total = total + (part[:, :128] * part[:, :128] + part[:, 128:] * part[:, 128:])
        squares[k] = total
        return parts

    def exchange(ref, k, slot, peer_of, conditions=None):
        copies = []
        for d in (1, 2, 3):
            sends, receives = (None, None) if conditions is None else conditions[d]
            copies.append(Copy(ref.at[k, slot], ref.at[k, slot], peer_of(d), sends, receives))
        return copies

    def prefixes(ref, k, matrices, where, slot, total=True):
        running = ref[k, 0]
        prefix[where, 0] = jnp.zeros((RHS, BAND), F32)
        prefix[where, 1] = running
        for q in (1, 2, 3):
            if q == 3 and not total:
                return None
            running = times_pair(running, *matrices(q)) + ref[k, q]
            if q < 3:
                prefix[where, q + 1] = running
        return running

    y_conditions = {d: (iy + d < 4, iy >= d) for d in (1, 2, 3)}
    y_matrix_conditions = {
        1: (jnp.logical_and(iy >= 1, iy <= 2), iy >= 2),
        2: (iy == 1, iy == 3),
        3: (False, False),
    }

    for k in range(ITERS):
        parts = residual(k, edges)
        if k == 0:
            loads["inv"].wait()
        whole = jnp.concatenate([rounded(part) for part in parts], axis=1)
        top_block = dot(whole, inv[:, :BAND])
        local[k, :, :BAND] = top_block
        top_copy = to_before(local.at[k, :, :BAND], next_top.at[k])
        bottom_block = dot(whole, inv[:, last])
        if k == 0:
            up_copy.arrived()
        shift = -times_exact(top_block, up_before[...])
        vc[k, core] = bottom_block - times_exact(shift, pair_mat[core])
        pair_vector = Copy(vc.at[k, core], vc.at[k, core], partner)
        local[k, :, BAND : COLS - BAND] = dot(whole, inv[:, BAND : COLS - BAND])
        pair_vector.arrived()
        vx[k, ix] = vc[k, 1] - times_exact(vc[k, 0], pair_mat[1])
        x_copies = exchange(vx, k, ix, on_x)
        if k == 0:
            pass_on(gx, ix, x_matrices)
            m, two, total = products(gx, mpx)
            store_halves(gz, iz, total)
            z_matrices = send_matrix(gz, iz, on_z)
            store_prefixes(mpx, m, two)
        for copy in x_copies:
            copy.arrived()
        vz[k, iz] = prefixes(vx, k, lambda q: load_halves(gx, q), 0, ix)
        z_copies = exchange(vz, k, iz, on_z)
        if k == 0:
            pass_on(gz, iz, z_matrices)
            m, two, total = products(gz, mpz)
            store_halves(gy, iy, total)
            y_matrices = send_matrix(gy, iy, on_y, y_matrix_conditions)
            store_prefixes(mpz, m, two)
        for copy in z_copies:
            copy.arrived()
        vy[k, iy] = prefixes(vz, k, lambda q: load_halves(gz, q), 1, iz)
        y_copies = exchange(vy, k, iy, on_y, y_conditions)
        top_copy.arrived()
        after_top = next_top[k]
        offset = bottom_block - times_exact(after_top, up[:, last])
        if k == 0:
            low_copy.arrived()
            pass_on(gy, iy, y_matrices)
        for copy in y_copies:
            copy.arrived()
        prefixes(vy, k, lambda q: load_halves(gy, q), 2, iy, total=False)
        carried = prefix[2, iy]
        carried = prefix[1, iz] + times_pair(carried, mpz[iz, :BAND, :], mpz[iz, BAND:, :])
        carried = prefix[0, ix] + times_pair(carried, mpx[ix, :BAND, :], mpx[ix, BAND:, :])
        second = vc[k, 0] - times_exact(carried, pair_mat[0])
        carried = jnp.where(core == 0, carried, second)
        previous = carried + shift
        current = offset - times_exact(previous, pair_mat[core])
        top = after_top - times_exact(current, low_after[...])
        top_rounded, previous_rounded = rounded(top), rounded(previous)
        for m in (0, 3, 1, 2):
            cols = slice(m * BAND, (m + 1) * BAND)
            own = slice((m + 1) * BAND, (m + 2) * BAND)
            block = bottom_block if m == 3 else local[k, :, cols]
            block = block - dot(top_rounded, up[:, cols])
            block = block - dot(previous_rounded, low[:, cols])
            new = xp[k, :, own] + block
            xp[k + 1, :, own] = new
            if k == ITERS - 1:
                x_out[:, cols] = new
            if m == 3:
                edges = send_edges(k + 1)

    residual(ITERS, edges)
    ones = jnp.ones((8, 128), F32)
    contract = (((1,), (1,)), ((), ()))
    totals[3, 0] = jnp.zeros((8, 128), F32)
    for k in range(ITERS + 1):
        row = lax.dot_general(
            ones, squares[k], contract, precision=lax.Precision.HIGHEST, preferred_element_type=F32
        )
        totals[3, 0, k : k + 1, :RHS] = row[:1, :]

    totals[0, core] = totals[3, 0]
    copy = Copy(totals.at[0, core], totals.at[0, core], partner)
    copy.arrived()
    value = totals[0, 0] + totals[0, 1]
    for level, (slot, peer_of) in enumerate(((ix, on_x), (iz, on_z), (iy, on_y))):
        ref = totals if level == 0 else None
        totals[4 + level, slot] = value
        copies = [
            Copy(totals.at[4 + level, slot], totals.at[4 + level, slot], peer_of(d))
            for d in (1, 2, 3)
        ]
        for copy in copies:
            copy.arrived()
        value = (totals[4 + level, 0] + totals[4 + level, 1]) + (
            totals[4 + level, 2] + totals[4 + level, 3]
        )
    norm_out[...] = jnp.sqrt(value * (1.0 / ORDER))
    for copy in sent:
        copy.left()


def body(*args):
    any_space = pl.BlockSpec(memory_space=pl.ANY)
    vmem = pl.BlockSpec(memory_space=pltpu.VMEM)
    matrix4 = pltpu.VMEM((4, 2, BAND, BAND), BF16)
    prefix4 = pltpu.VMEM((4, 2 * BAND, BAND), BF16)
    vectors4 = pltpu.VMEM((ITERS, 4, RHS, BAND), F32)
    x, norms = pl.pallas_call(
        kernel,
        out_shape=(
            jax.ShapeDtypeStruct((RHS, COLS), F32),
            jax.ShapeDtypeStruct((8, 128), F32),
        ),
        in_specs=[any_space] * 8,
        out_specs=(vmem, vmem),
        scratch_shapes=[
            pltpu.VMEM((RHS, COLS), F32),
            pltpu.VMEM((COLS, BAND), F32),
            pltpu.VMEM((COLS, BAND), F32),
            pltpu.VMEM((COLS, BAND), F32),
            pltpu.VMEM((COLS, COLS), BF16),
            pltpu.VMEM((BAND, COLS), BF16),
            pltpu.VMEM((BAND, COLS), BF16),
            pltpu.VMEM((4, 3 * BAND, BAND), BF16),
            pltpu.VMEM((4, 3 * BAND, BAND), BF16),
            pltpu.VMEM((ITERS + 1, RHS, COLS + 2 * BAND), F32),
            pltpu.VMEM((2, BAND, BAND), BF16),
            pltpu.VMEM((BAND, BAND), BF16),
            pltpu.VMEM((BAND, BAND), BF16),
            matrix4,
            matrix4,
            matrix4,
            prefix4,
            prefix4,
            pltpu.VMEM((ITERS, RHS, COLS), F32),
            pltpu.VMEM((ITERS, RHS, BAND), F32),
            pltpu.VMEM((ITERS, 2, RHS, BAND), F32),
            vectors4,
            vectors4,
            vectors4,
            pltpu.VMEM((3, 4, RHS, BAND), F32),
            pltpu.VMEM((ITERS + 1, RHS, 128), F32),
            pltpu.VMEM((7, 4, 8, 128), F32),
            pltpu.SemaphoreType.DMA((16,)),
            pltpu.SemaphoreType.DMA((COPIES,)),
            pltpu.SemaphoreType.DMA((COPIES,)),
        ],
        compiler_params=pltpu.CompilerParams(collective_id=0, has_side_effects=True),
    )(*args)
    return x, norms[: ITERS + 1, :RHS]


def solution(mesh):
    cols, rows = P(None, "rows"), P("rows", None)
    return jax.shard_map(
        body,
        mesh=mesh,
        in_specs=(cols, cols, rows, rows, rows, rows, cols, cols),
        out_specs=(cols, P()),
        check_vma=False,
    )
```
